256 devices in a mesh: lon: 16 (over z, core), lat: 16 (over y, x).
Axes of the slice: x: 4, y: 4, z: 8, core: 2. Of those that a mesh axis runs over, the one named last changes fastest.
Arguments:
- wave_action: float32 [256, 128, 1152], P('lon', 'lat'), may hold values from -6 to 6
- lon_speed: float32 [256, 128, 1152], P('lon', 'lat'), may hold values from 4 to 128
- lat_speed: float32 [256, 128, 1152], P('lon', 'lat'), may hold values from 4 to 128
- land_mask: int32 [256, 128], P('lon', 'lat'), may hold values 0 or 1
- open_edges: int32 [2, 256], P(None, 'lon'), may hold values 0 or 1
Outputs:
- propagated: float32 [256, 128, 1152], P('lon', 'lat')
The draws below stay inside these ranges and needn't reach their ends.
All inputs are finite; a program needn't handle non-finite values. No bound on the sum of `land_mask` or of `open_edges` on one device may be relied on, other than what follows from the above.
Results may differ from the reference program's by a relative error of at most 0.00002.
Values sent between devices are 32-bit elements; how exact they have to be, the bound alone decides.
No kernel may reach another device: no remote copies, remote signals or barrier semaphores. Data moves between devices by JAX's collectives and lax.ppermute only.
A program may use at most 64 MiB of HBM per device.

```python
import math
import jax
import jax.numpy as jnp
from jax import lax

ND = 36
NB = 1152
NX = 256
NY = 128


def place_ends(entries, key, smallest, largest):
    extent = entries.shape
    place = [jax.random.randint(jax.random.fold_in(key, axis), (), 0, extent[axis]) for axis in range(len(extent))]
    entries = entries.at[tuple(place)].set(smallest)
    longest = extent.index(max(extent))
    place[longest] = (place[longest] + 1) % extent[longest]
    return entries.at[tuple(place)].set(largest)


def block_scale(key, shape, split, smallest, top_value):
    level = 1.0
    for dim, blocks in split:
        heights = jax.random.uniform(jax.random.fold_in(jax.random.fold_in(key, 6), dim), (blocks,), jnp.float32, smallest / len(split), top_value / len(split))
        level = level * jnp.repeat(jnp.exp(heights), shape[dim] // blocks).reshape((-1,) + (1,) * (len(shape) - 1 - dim))
    return level


def normal_values(stream_key, shape, spread, reach, shards=(), kind=jnp.bfloat16):
    array = jax.random.normal(stream_key, shape, jnp.float32) * spread
    if len(shards) > 0:
        array = block_scale(stream_key, shape, shards, -0.22, 0.18) * array
    return jnp.clip(array, min=-reach, max=reach).astype(kind)


def setup_inputs(seed: int = 0) -> dict:
    splits = jax.random.split(jax.random.key(seed), 6)
    wave_action = normal_values(splits[0], (NX, NY, NB), 1.0, 6.0, ((0, 16), (1, 16)), jnp.float32)
    lon_speed = jnp.clip(jnp.exp(math.log(128.0) - 3.465736 * jax.random.uniform(splits[1], (NX, NY, NB), jnp.float32) ** block_scale(splits[1], (NX, NY, NB), ((0, 16), (1, 16)), -0.2, 0.2)), 4.0, 128.0)
    lat_speed = jnp.clip(jnp.exp(math.log(128.0) - 3.465736 * jax.random.uniform(splits[2], (NX, NY, NB), jnp.float32) ** block_scale(splits[2], (NX, NY, NB), ((0, 16), (1, 16)), -0.2, 0.2)), 4.0, 128.0)
    land_mask = place_ends((jax.random.randint(splits[3], (NX, NY), 0, 64) < 63).astype(jnp.int32), jax.random.fold_in(splits[3], 1), 0, 1)
    open_edges = place_ends((jax.random.randint(splits[4], (2, NX), 0, 2) < 1).astype(jnp.int32), jax.random.fold_in(splits[4], 1), 0, 1)
    return dict(wave_action=wave_action, lon_speed=lon_speed, lat_speed=lat_speed, land_mask=land_mask, open_edges=open_edges)


def bin_angles(bin_count):
    direction = jnp.arange(bin_count, dtype=jnp.int32) % ND
    heading = (direction.astype(jnp.float32) + 0.5) * (2.0 * jnp.pi / ND)
    return jnp.cos(heading), jnp.sin(heading)


def upwind_parts(flow):
    return jnp.maximum(flow, 0.0), jnp.maximum(-flow, 0.0)


def sweep_solve(sub_band, main_band, super_band, right_side):
    zeros_row = jnp.zeros_like(right_side[0])

    def forward_step(carried, row_data):
        ratio_prev, value_prev = carried
        sub_row, main_row, super_row, rhs_row = row_data
        pivot = main_row - sub_row * ratio_prev
        result = (super_row / pivot, (rhs_row - sub_row * value_prev) / pivot)
        return result, result

    _, (ratios, partial_values) = lax.scan(forward_step, (zeros_row, zeros_row), (sub_band, main_band, super_band, right_side))

    def backward_step(carried, row_data):
        ratio_row, value_row = row_data
        result = value_row - ratio_row * carried
        return result, result

    _, solution = lax.scan(backward_step, zeros_row, (ratios, partial_values), reverse=True)
    return solution


def cyclic_solve(sub_band, main_band, super_band, right_side):
    head_rows = right_side.shape[0] - 1
    row_order = lax.broadcasted_iota(jnp.int32, (head_rows, 1, 1), 0)
    coupled = jnp.where(row_order == 0, sub_band[:head_rows], 0.0) + jnp.where(row_order == head_rows - 1, super_band[:head_rows], 0.0)
    base_part = sweep_solve(sub_band[:head_rows], main_band[:head_rows], super_band[:head_rows], right_side[:head_rows])
    tail_part = sweep_solve(sub_band[:head_rows], main_band[:head_rows], super_band[:head_rows], coupled)
    numerator = right_side[head_rows] - sub_band[head_rows] * base_part[head_rows - 1] - super_band[head_rows] * base_part[0]
    denominator = main_band[head_rows] - sub_band[head_rows] * tail_part[head_rows - 1] - super_band[head_rows] * tail_part[0]
    last_value = numerator / denominator
    return jnp.concatenate([base_part - tail_part * last_value[None], last_value[None]], 0)


def reference(wave_action, lon_speed, lat_speed, land_mask, open_edges):
    cosines, sine_terms = bin_angles(wave_action.shape[2])
    sea_mask = land_mask.astype(jnp.float32)[:, :, None]
    source = wave_action * sea_mask
    onward, backward = upwind_parts(lon_speed * cosines * sea_mask)
    halfway = cyclic_solve(-onward, 1.0 + onward + backward, -backward, source)
    onward, backward = upwind_parts(jnp.moveaxis(lat_speed * sine_terms * sea_mask, 1, 0))
    opened = open_edges.astype(jnp.float32)
    main_band = 1.0 + onward + backward
    main_band = main_band.at[0].set(1.0 + backward[0] + onward[0] * opened[0][:, None])
    main_band = main_band.at[-1].set(1.0 + onward[-1] + backward[-1] * opened[1][:, None])
    result = sweep_solve(-onward, main_band, -backward, jnp.moveaxis(halfway, 1, 0))
    return jnp.moveaxis(result, 0, 1)
```

```python
import jax
import jax.numpy as jnp
import numpy as np
from jax import lax
from jax.experimental import pallas as pl
from jax.experimental.pallas import tpu as pltpu
from jax.sharding import PartitionSpec as P

ND = 36
HALF = ND // 2
LANES = 128
CHUNK = 3 * LANES


def bin_tables(bins):
    heading = ((np.arange(bins) % ND).astype(np.float32) + np.float32(0.5)) * np.float32(2.0 * np.pi / ND)
    cosines, sines = np.cos(heading), np.sin(heading)
    rows = [np.abs(cosines), np.abs(sines), cosines > 0, sines > 0]
    return np.stack([np.asarray(row, np.float32) for row in rows] + [np.zeros(bins, np.float32)] * 4)


def chunks(bins):
    step = CHUNK if bins % CHUNK == 0 else bins
    return [slice(start, start + step) for start in range(0, bins, step)]


def tiles_of(part):
    return range(part.start // LANES, part.stop // LANES)


def take(ref, rows, part, start, size, stride=1):
    picked = [ref[pl.ds(tile * rows + start, size, stride=stride), :] for tile in tiles_of(part)]
    return jnp.concatenate(picked, axis=1)


def put(ref, rows, part, start, value, stride=1):
    for n, tile in enumerate(tiles_of(part)):
        place = pl.ds(tile * rows + start, value.shape[0], stride=stride)
        ref[place, :] = value[:, n * LANES : (n + 1) * LANES]


def compose(first, second):
    return second[0] * first[0], second[0] * first[1] + second[1]


def lon_local(wave, speed, mask, table, message, partial, decay):
    count, lats = mask.shape
    rows = count * lats
    sea = mask[...].astype(jnp.float32).T
    for part in chunks(wave.shape[1]):
        cosine, east = table[0:1, part], table[2:3, part] > 0.5

        def row(i):
            water = sea[:, i : i + 1]
            flow = speed[i * lats : (i + 1) * lats, part] * cosine * water
            scale = 1.0 / (1.0 + flow)
            return flow * scale, wave[i * lats : (i + 1) * lats, part] * water * scale

        value = total = None
        for k in range(count):
            if k < count // 2:
                a_low, b_low = row(k)
                a_high, b_high = row(count - 1 - k)
                there = (count - 1 - k) * lats
                put(decay, rows, part, there, jnp.where(east, a_high, a_low))
                put(partial, rows, part, there, jnp.where(east, b_high, b_low))
                a, b = jnp.where(east, a_low, a_high), jnp.where(east, b_low, b_high)
            else:
                a = take(decay, rows, part, k * lats, lats)
                b = take(partial, rows, part, k * lats, lats)
            value = b if k == 0 else a * value + b
            total = a if k == 0 else a * total
            put(partial, rows, part, k * lats, value)
            put(decay, rows, part, k * lats, total)
        message[0:lats, part] = total
        message[lats : 2 * lats, part] = value


def lat_coefficients(speed, mask, edges, table, ratio, scaled, decay, rate, arrived):
    lons, count = mask.shape
    rows = lons * count
    parts = chunks(speed.shape[1])

    def copy(tile):
        lanes = pl.ds(tile * LANES, LANES)
        return pltpu.make_async_copy(
            speed.at[:, lanes], rate.at[pl.ds(tile * rows, rows), :], arrived.at[tile]
        )

    for part in parts:
        for tile in tiles_of(part):
            copy(tile).start()
    place, last = lax.axis_index("lat"), lax.axis_size("lat") - 1
    sea = mask[...].astype(jnp.float32)
    opened = edges[...].astype(jnp.float32).T
    south = jnp.where(place == 0, opened[:, 0:1], 1.0)
    north = jnp.where(place == last, opened[:, 1:2], 1.0)
    for part in parts:
        for tile in tiles_of(part):
            copy(tile).wait()
        sine, up = table[1:2, part], table[3:4, part] > 0.5
        flows = [
            take(rate, rows, part, j, lons, count) * sine * sea[:, j : j + 1] for j in range(count)
        ]
        total = None
        for k in range(count):
            flow = jnp.where(up, flows[k], flows[count - 1 - k])
            shown = flow * jnp.where(up, south, north) if k == 0 else flow
            scale = 1.0 / (1.0 + shown)
            a = flow * scale
            total = a if k == 0 else a * total
            put(ratio, rows, part, k * lons, a)
            put(scaled, rows, part, k * lons, scale)
            put(decay, rows, part, k * lons, total)


def ordered_group(own, received, place, positive):
    members = [own, *received]
    in_place = []
    for slot in range(4):
        value = members[0]
        for d in range(1, 4):
            hit = (place + 4 - slot) % 4 == d
            value = [jnp.where(hit, new, old) for new, old in zip(members[d], value)]
        in_place.append(value)
    swept = [
        [jnp.where(positive, low, high) for low, high in zip(in_place[slot], in_place[3 - slot])]
        for slot in range(4)
    ]
    prefixes = [[jnp.ones_like(own[0]), jnp.zeros_like(own[1])], swept[0]]
    prefixes.append(compose(swept[0], swept[1]))
    prefixes.append(compose(prefixes[2], swept[2]))
    whole = compose(prefixes[3], swept[3])

    def chosen(index):
        value = prefixes[0]
        for slot in range(1, 4):
            value = [jnp.where(index == slot, new, old) for new, old in zip(prefixes[slot], value)]
        return value

    before = [jnp.where(positive, low, high) for low, high in zip(chosen(place), chosen(3 - place))]
    return whole, before


def halves(ref, part):
    rows = ref.shape[0] // 2
    return [ref[0:rows, part], ref[rows : 2 * rows, part]]


def lon_group(own, first, second, third, table, whole, before):
    place = lax.axis_index("lon") % 4
    rows = own.shape[0] // 2
    for part in chunks(own.shape[1]):
        received = [halves(ref, part) for ref in (first, second, third)]
        total, prefix = ordered_group(halves(own, part), received, place, table[2:3, part] > 0.5)
        whole[0:rows, part], whole[rows : 2 * rows, part] = total
        before[0:rows, part], before[rows : 2 * rows, part] = prefix


def lon_finish(
    partial, decay, own, first, second, third, before, ratio, scaled, lat_decay, table,
    message, solved, half,
):
    lats, lons = own.shape[0] // 2, message.shape[0] // 2
    rows = lons * lats
    for part in chunks(own.shape[1]):
        east, up = table[2:3, part] > 0.5, table[3:4, part] > 0.5
        one, two, three = (halves(ref, part) for ref in (first, second, third))
        cycle = halves(own, part)
        cycle = compose(cycle, [jnp.where(east, x, y) for x, y in zip(three, one)])
        cycle = compose(cycle, two)
        cycle = compose(cycle, [jnp.where(east, x, y) for x, y in zip(one, three)])
        entering = cycle[1] / (1.0 - cycle[0])
        prefix = halves(before, part)
        entering = prefix[0] * entering + prefix[1]
        for k in range(lons // 2):
            low, high = k * lats, (lons - 1 - k) * lats
            a, b = (
                take(partial, rows, part, at, lats) + take(decay, rows, part, at, lats) * entering
                for at in (low, high)
            )
            put(half, rows, part, low, jnp.where(east, a, b))
            put(half, rows, part, high, jnp.where(east, b, a))
        lines = [take(half, rows, part, j, lons, lats) for j in range(lats)]
        value = None
        for k in range(lats):
            step = take(scaled, rows, part, k * lons, lons)
            step = step * jnp.where(up, lines[k], lines[lats - 1 - k])
            value = step if k == 0 else take(ratio, rows, part, k * lons, lons) * value + step
            put(solved, rows, part, k * lons, value)
        message[0:lons, part] = take(lat_decay, rows, part, (lats - 1) * lons, lons)
        message[lons : 2 * lons, part] = value


def lat_group(own, first, second, third, table, before, *messages):
    place = lax.axis_index("lat")
    rows = own.shape[0] // 2
    everything = slice(0, own.shape[1])
    received = [halves(ref, everything) for ref in (first, second, third)]
    up = table[3:4, :] > 0.5
    total, prefix = ordered_group(halves(own, everything), received, place % 4, up)
    before[0:rows], before[rows : 2 * rows] = prefix
    turned = pltpu.roll(total[1], HALF, 1)
    north, south = jnp.where(up, total[0], turned), jnp.where(up, turned, total[0])
    for d, message in enumerate(messages, 1):
        message[...] = jnp.where(place // 4 + d < 4, north, south)


def lat_finish(solved, decay, before, first, second, third, table, out, result, sent):
    lons, bins = before.shape[0] // 2, before.shape[1]
    rows = out.shape[0]
    count = rows // lons
    row = lax.axis_index("lat") // 4
    up = table[3:4, :] > 0.5
    one, two, three = ((ref[...], pltpu.roll(ref[...], bins - HALF, 1)) for ref in (first, second, third))
    entering = jnp.zeros_like(one[0])
    for d, low, high in ((3, three, one), (2, two, two), (1, one, three)):
        a, b = (jnp.where(up, x, y) for x, y in zip(low, high))
        reached = jnp.where(up, (row >= d).astype(jnp.float32), (row < 4 - d).astype(jnp.float32))
        entering = jnp.where(reached > 0.5, a * entering + b, entering)
    entering = before[0:lons] * entering + before[lons : 2 * lons]
    copies = []
    for part in chunks(bins):
        goes_up, inflow = up[:, part], entering[:, part]
        for k in range(count // 2):
            low, high = k * lons, (count - 1 - k) * lons
            a, b = (
                take(solved, rows, part, at, lons) + take(decay, rows, part, at, lons) * inflow
                for at in (low, high)
            )
            put(result, rows, part, k, jnp.where(goes_up, a, b), count)
            put(result, rows, part, count - 1 - k, jnp.where(goes_up, b, a), count)
        for tile in tiles_of(part):
            copy = pltpu.make_async_copy(
                result.at[pl.ds(tile * rows, rows), :],
                out.at[:, pl.ds(tile * LANES, LANES)],
                sent.at[tile],
            )
            copy.start()
            copies.append(copy)
    for copy in copies:
        copy.wait()


def run(kernel, shapes, *operands, scratch=(), far_inputs=(), far_outputs=()):
    here, away = pl.BlockSpec(memory_space=pltpu.VMEM), pl.BlockSpec(memory_space=pl.ANY)
    return pl.pallas_call(
        kernel,
        out_shape=[jax.ShapeDtypeStruct(shape, jnp.float32) for shape in shapes],
        in_specs=[away if n in far_inputs else here for n in range(len(operands))],
        out_specs=[away if n in far_outputs else here for n in range(len(shapes))],
        scratch_shapes=scratch,
        name=kernel.__name__,
    )(*operands)


def exchange(value, axis, near):
    def route(d):
        pairs = []
        for i in range(16):
            base, k = (i - i % 4, i % 4) if near else (i % 4, i // 4)
            source = (k - d) % 4
            pairs.append((base + source if near else base + 4 * source, i))
        return pairs

    values = value if isinstance(value, list) else [value] * 3
    return [lax.ppermute(item, axis, route(d)) for d, item in enumerate(values, 1)]


def body(wave_action, lon_speed, lat_speed, land_mask, open_edges):
    lons, lats, bins = wave_action.shape
    table = jnp.asarray(bin_tables(bins))
    flat = (lons * lats, bins)
    wave, speed, lat_rate = (x.reshape(flat) for x in (wave_action, lon_speed, lat_speed))
    small, large = (2 * lats, bins), (2 * lons, bins)

    tiled = (bins // LANES * lons * lats, LANES)
    buffer = pltpu.VMEM(tiled, jnp.float32)
    signals = pltpu.SemaphoreType.DMA((bins // LANES,))

    own, partial, decay = run(lon_local, [small, tiled, tiled], wave, speed, land_mask, table)
    near = exchange(own, "lon", True)
    ratio, scaled, lat_decay = run(
        lat_coefficients, [tiled] * 3, lat_rate, land_mask, open_edges, table,
        scratch=[buffer, signals], far_inputs=(0,),
    )
    whole, before = run(lon_group, [small, small], own, *near, table)
    far = exchange(whole, "lon", False)
    lat_own, solved = run(
        lon_finish, [large, tiled],
        partial, decay, whole, *far, before, ratio, scaled, lat_decay, table,
        scratch=[buffer],
    )
    near = exchange(lat_own, "lat", True)
    lat_before, *sends = run(lat_group, [large, *[(lons, bins)] * 3], lat_own, *near, table)
    far = exchange(list(sends), "lat", False)
    (out,) = run(
        lat_finish, [flat], solved, lat_decay, lat_before, *far, table,
        scratch=[buffer, signals], far_outputs=(0,),
    )
    return out.reshape(wave_action.shape)


def solution(mesh):
    return jax.shard_map(
        body,
        mesh=mesh,
        in_specs=(
            P("lon", "lat", None),
            P("lon", "lat", None),
            P("lon", "lat", None),
            P("lon", "lat"),
            P(None, "lon"),
        ),
        out_specs=P("lon", "lat", None),
        check_vma=False,
    )
```

```python
import jax
import jax.numpy as jnp
import numpy as np
from jax import lax
from jax.experimental import pallas as pl
from jax.experimental.pallas import tpu as pltpu
from jax.sharding import PartitionSpec as P

ND = 36
HALF = ND // 2
LANES = 128
CHUNK = 3 * LANES


def bin_tables(bins):
    heading = ((np.arange(bins) % ND).astype(np.float32) + np.float32(0.5)) * np.float32(2.0 * np.pi / ND)
    cosines, sines = np.cos(heading), np.sin(heading)
    rows = [np.abs(cosines), np.abs(sines), cosines > 0, sines > 0]
    return np.stack([np.asarray(row, np.float32) for row in rows] + [np.zeros(bins, np.float32)] * 4)


def chunks(bins):
    step = CHUNK if bins % CHUNK == 0 else bins
    return [slice(start, start + step) for start in range(0, bins, step)]


def tiles_of(part):
    return range(part.start // LANES, part.stop // LANES)


def take(ref, rows, part, start, size, stride=1):
    picked = [ref[pl.ds(tile * rows + start, size, stride=stride), :] for tile in tiles_of(part)]
    return jnp.concatenate(picked, axis=1)


def put(ref, rows, part, start, value, stride=1):
    for n, tile in enumerate(tiles_of(part)):
        place = pl.ds(tile * rows + start, value.shape[0], stride=stride)
        ref[place, :] = value[:, n * LANES : (n + 1) * LANES]


def compose(first, second):
    return second[0] * first[0], second[0] * first[1] + second[1]


def lon_local(
    wave_far, speed_far, mask_far, table_far, message, partial, decay,
    wave, speed, mask, table, arrived,
):
    lats, count = mask.shape
    rows = count * lats
    parts = chunks(wave.shape[1])
    small = [
        pltpu.make_async_copy(mask_far, mask, arrived.at[0]),
        pltpu.make_async_copy(table_far, table, arrived.at[1]),
    ]
    large = [
        [
            pltpu.make_async_copy(far.at[:, part], near.at[:, part], arrived.at[2 * n + which])
            for which, (far, near) in enumerate(((wave_far, wave), (speed_far, speed)))
        ]
        for n, part in enumerate(parts, 1)
    ]
    for copies in (small, *large):
        for copy in copies:
            copy.start()
    for copy in small:
        copy.wait()
    sea = mask[...].astype(jnp.float32)
    for part, copies in zip(parts, large):
        for copy in copies:
            copy.wait()
        cosine, east = table[0:1, part], table[2:3, part] > 0.5

        def row(i):
            water = sea[:, i : i + 1]
            flow = speed[i * lats : (i + 1) * lats, part] * cosine * water
            scale = 1.0 / (1.0 + flow)
            return flow * scale, wave[i * lats : (i + 1) * lats, part] * water * scale

        value = total = None
        for k in range(count):
            if k < count // 2:
                a_low, b_low = row(k)
                a_high, b_high = row(count - 1 - k)
                there = (count - 1 - k) * lats
                put(decay, rows, part, there, jnp.where(east, a_high, a_low))
                put(partial, rows, part, there, jnp.where(east, b_high, b_low))
                a, b = jnp.where(east, a_low, a_high), jnp.where(east, b_low, b_high)
            else:
                a = take(decay, rows, part, k * lats, lats)
                b = take(partial, rows, part, k * lats, lats)
            value = b if k == 0 else a * value + b
            total = a if k == 0 else a * total
            put(partial, rows, part, k * lats, value)
            put(decay, rows, part, k * lats, total)
        message[0:lats, part] = total
        message[lats : 2 * lats, part] = value


def lat_coefficients(speed, mask, edges, table, ratio, scaled, decay, rate):
    count, lons = mask.shape
    rows = lons * count
    place, last = lax.axis_index("lat"), lax.axis_size("lat") - 1
    sea = mask[...].astype(jnp.float32).T
    opened = edges[...].astype(jnp.float32).T
    south = jnp.where(place == 0, opened[:, 0:1], 1.0)
    north = jnp.where(place == last, opened[:, 1:2], 1.0)
    for part in chunks(speed.shape[1]):
        put(rate, rows, part, 0, speed[:, part])
        sine, up = table[1:2, part], table[3:4, part] > 0.5
        flows = [
            take(rate, rows, part, j, lons, count) * sine * sea[:, j : j + 1] for j in range(count)
        ]
        total = None
        for k in range(count):
            flow = jnp.where(up, flows[k], flows[count - 1 - k])
            shown = flow * jnp.where(up, south, north) if k == 0 else flow
            scale = 1.0 / (1.0 + shown)
            a = flow * scale
            total = a if k == 0 else a * total
            put(ratio, rows, part, k * lons, a)
            put(scaled, rows, part, k * lons, scale)
            put(decay, rows, part, k * lons, total)


def ordered_group(own, received, place, positive):
    members = [own, *received]
    in_place = []
    for slot in range(4):
        value = members[0]
        for d in range(1, 4):
            hit = (place + 4 - slot) % 4 == d
            value = [jnp.where(hit, new, old) for new, old in zip(members[d], value)]
        in_place.append(value)
    swept = [
        [jnp.where(positive, low, high) for low, high in zip(in_place[slot], in_place[3 - slot])]
        for slot in range(4)
    ]
    prefixes = [[jnp.ones_like(own[0]), jnp.zeros_like(own[1])], swept[0]]
    prefixes.append(compose(swept[0], swept[1]))
    prefixes.append(compose(prefixes[2], swept[2]))
    whole = compose(prefixes[3], swept[3])

    def chosen(index):
        value = prefixes[0]
        for slot in range(1, 4):
            value = [jnp.where(index == slot, new, old) for new, old in zip(prefixes[slot], value)]
        return value

    before = [jnp.where(positive, low, high) for low, high in zip(chosen(place), chosen(3 - place))]
    return whole, before


def halves(ref, part):
    rows = ref.shape[0] // 2
    return [ref[0:rows, part], ref[rows : 2 * rows, part]]


def lon_group(own, first, second, third, table, whole, before):
    place = lax.axis_index("lon") % 4
    rows = own.shape[0] // 2
    for part in chunks(own.shape[1]):
        received = [halves(ref, part) for ref in (first, second, third)]
        total, prefix = ordered_group(halves(own, part), received, place, table[2:3, part] > 0.5)
        whole[0:rows, part], whole[rows : 2 * rows, part] = total
        before[0:rows, part], before[rows : 2 * rows, part] = prefix


def lon_finish(
    partial, decay, own, first, second, third, before, ratio, scaled, lat_decay, table,
    message, solved, half,
):
    lats, lons = own.shape[0] // 2, message.shape[0] // 2
    rows = lons * lats
    for part in chunks(own.shape[1]):
        east, up = table[2:3, part] > 0.5, table[3:4, part] > 0.5
        one, two, three = (halves(ref, part) for ref in (first, second, third))
        cycle = halves(own, part)
        cycle = compose(cycle, [jnp.where(east, x, y) for x, y in zip(three, one)])
        cycle = compose(cycle, two)
        cycle = compose(cycle, [jnp.where(east, x, y) for x, y in zip(one, three)])
        entering = cycle[1] / (1.0 - cycle[0])
        prefix = halves(before, part)
        entering = prefix[0] * entering + prefix[1]
        for k in range(lons // 2):
            low, high = k * lats, (lons - 1 - k) * lats
            a, b = (
                take(partial, rows, part, at, lats) + take(decay, rows, part, at, lats) * entering
                for at in (low, high)
            )
            put(half, rows, part, low, jnp.where(east, a, b))
            put(half, rows, part, high, jnp.where(east, b, a))
        lines = [take(half, rows, part, j, lons, lats) for j in range(lats)]
        value = None
        for k in range(lats):
            step = take(scaled, rows, part, k * lons, lons)
            step = step * jnp.where(up, lines[k], lines[lats - 1 - k])
            value = step if k == 0 else take(ratio, rows, part, k * lons, lons) * value + step
            put(solved, rows, part, k * lons, value)
        message[0:lons, part] = take(lat_decay, rows, part, (lats - 1) * lons, lons)
        message[lons : 2 * lons, part] = value


def lat_group(own, first, second, third, table, before, *messages):
    place = lax.axis_index("lat")
    rows = own.shape[0] // 2
    everything = slice(0, own.shape[1])
    received = [halves(ref, everything) for ref in (first, second, third)]
    up = table[3:4, :] > 0.5
    total, prefix = ordered_group(halves(own, everything), received, place % 4, up)
    before[0:rows], before[rows : 2 * rows] = prefix
    turned = pltpu.roll(total[1], HALF, 1)
    north, south = jnp.where(up, total[0], turned), jnp.where(up, turned, total[0])
    for d, message in enumerate(messages, 1):
        message[...] = jnp.where(place // 4 + d < 4, north, south)


def lat_finish(solved, decay, before, first, second, third, table, out, result, sent):
    lons, bins = before.shape[0] // 2, before.shape[1]
    rows = out.shape[0]
    count = rows // lons
    row = lax.axis_index("lat") // 4
    up = table[3:4, :] > 0.5
    one, two, three = ((ref[...], pltpu.roll(ref[...], bins - HALF, 1)) for ref in (first, second, third))
    entering = jnp.zeros_like(one[0])
    for d, low, high in ((3, three, one), (2, two, two), (1, one, three)):
        a, b = (jnp.where(up, x, y) for x, y in zip(low, high))
        reached = jnp.where(up, (row >= d).astype(jnp.float32), (row < 4 - d).astype(jnp.float32))
        entering = jnp.where(reached > 0.5, a * entering + b, entering)
    entering = before[0:lons] * entering + before[lons : 2 * lons]
    copies = []
    for part in chunks(bins):
        goes_up, inflow = up[:, part], entering[:, part]
        for k in range(count // 2):
            low, high = k * lons, (count - 1 - k) * lons
            a, b = (
                take(solved, rows, part, at, lons) + take(decay, rows, part, at, lons) * inflow
                for at in (low, high)
            )
            put(result, rows, part, k, jnp.where(goes_up, a, b), count)
            put(result, rows, part, count - 1 - k, jnp.where(goes_up, b, a), count)
        for tile in tiles_of(part):
            copy = pltpu.make_async_copy(
                result.at[pl.ds(tile * rows, rows), :],
                out.at[:, pl.ds(tile * LANES, LANES)],
                sent.at[tile],
            )
            copy.start()
            copies.append(copy)
    for copy in copies:
        copy.wait()


def run(kernel, shapes, *operands, scratch=(), far_inputs=(), far_outputs=()):
    here, away = pl.BlockSpec(memory_space=pltpu.VMEM), pl.BlockSpec(memory_space=pltpu.HBM)
    operands = [
        pltpu.with_memory_space_constraint(x, pltpu.HBM) if n in far_inputs else x
        for n, x in enumerate(operands)
    ]
    return pl.pallas_call(
        kernel,
        out_shape=[jax.ShapeDtypeStruct(shape, jnp.float32) for shape in shapes],
        in_specs=[away if n in far_inputs else here for n in range(len(operands))],
        out_specs=[away if n in far_outputs else here for n in range(len(shapes))],
        scratch_shapes=scratch,
        compiler_params=pltpu.CompilerParams(vmem_limit_bytes=8 << 20),
        name=kernel.__name__,
    )(*operands)


def exchange(value, axis, near):
    def route(d):
        pairs = []
        for i in range(16):
            base, k = (i - i % 4, i % 4) if near else (i % 4, i // 4)
            source = (k - d) % 4
            pairs.append((base + source if near else base + 4 * source, i))
        return pairs

    values = value if isinstance(value, list) else [value] * 3
    return [lax.ppermute(item, axis, route(d)) for d, item in enumerate(values, 1)]


def body(wave_action, lon_speed, lat_speed, land_mask, open_edges):
    lons, lats, bins = wave_action.shape
    table = jnp.asarray(bin_tables(bins))
    flat = (lons * lats, bins)
    wave, speed, lat_rate = (x.reshape(flat) for x in (wave_action, lon_speed, lat_speed))
    small, large = (2 * lats, bins), (2 * lons, bins)

    tiled = (bins // LANES * lons * lats, LANES)
    buffer = pltpu.VMEM(tiled, jnp.float32)
    signals = pltpu.SemaphoreType.DMA((bins // LANES,))

    sea = land_mask.T
    own, partial, decay = run(
        lon_local, [small, tiled, tiled], wave, speed, sea, table,
        scratch=[
            pltpu.VMEM(flat, jnp.float32), pltpu.VMEM(flat, jnp.float32),
            pltpu.VMEM(sea.shape, sea.dtype), pltpu.VMEM(table.shape, table.dtype),
            pltpu.SemaphoreType.DMA((2 + 2 * len(chunks(bins)),)),
        ],
        far_inputs=range(4),
    )
    near = exchange(own, "lon", True)
    ratio, scaled, lat_decay = run(
        lat_coefficients, [tiled] * 3, lat_rate, sea, open_edges, table, scratch=[buffer]
    )
    whole, before = run(lon_group, [small, small], own, *near, table)
    far = exchange(whole, "lon", False)
    lat_own, solved = run(
        lon_finish, [large, tiled],
        partial, decay, whole, *far, before, ratio, scaled, lat_decay, table,
        scratch=[buffer],
    )
    near = exchange(lat_own, "lat", True)
    lat_before, *sends = run(lat_group, [large, *[(lons, bins)] * 3], lat_own, *near, table)
    far = exchange(list(sends), "lat", False)
    (out,) = run(
        lat_finish, [flat], solved, lat_decay, lat_before, *far, table,
        scratch=[buffer, signals], far_outputs=(0,),
    )
    return out.reshape(wave_action.shape)


def solution(mesh):
    return jax.shard_map(
        body,
        mesh=mesh,
        in_specs=(
            P("lon", "lat", None),
            P("lon", "lat", None),
            P("lon", "lat", None),
            P("lon", "lat"),
            P(None, "lon"),
        ),
        out_specs=P("lon", "lat", None),
        check_vma=False,
    )
```

```python
import jax
import jax.numpy as jnp
import numpy as np
from jax import lax
from jax.experimental import pallas as pl
from jax.experimental.pallas import tpu as pltpu
from jax.sharding import PartitionSpec as P

ND = 36
HALF = ND // 2
LANES = 128
CHUNK = 3 * LANES


def bin_tables(bins):
    heading = ((np.arange(bins) % ND).astype(np.float32) + np.float32(0.5)) * np.float32(2.0 * np.pi / ND)
    cosines, sines = np.cos(heading), np.sin(heading)
    rows = [np.abs(cosines), np.abs(sines), cosines > 0, sines > 0]
    return np.stack([np.asarray(row, np.float32) for row in rows] + [np.zeros(bins, np.float32)] * 4)


def chunks(bins):
    step = CHUNK if bins % CHUNK == 0 else bins
    return [slice(start, start + step) for start in range(0, bins, step)]


def tiles_of(part):
    return range(part.start // LANES, part.stop // LANES)


def take(ref, rows, part, start, size, stride=1):
    picked = [ref[pl.ds(tile * rows + start, size, stride=stride), :] for tile in tiles_of(part)]
    return jnp.concatenate(picked, axis=1)


def put(ref, rows, part, start, value, stride=1):
    for n, tile in enumerate(tiles_of(part)):
        place = pl.ds(tile * rows + start, value.shape[0], stride=stride)
        ref[place, :] = value[:, n * LANES : (n + 1) * LANES]


def compose(first, second):
    return second[0] * first[0], second[0] * first[1] + second[1]


def lon_local(
    wave_far, speed_far, mask_far, table_far, keep, give, partial, decay,
    wave, speed, mask, table, arrived,
):
    lats, count = mask.shape
    rows = count * lats
    parts = chunks(wave.shape[1])
    small = [
        pltpu.make_async_copy(mask_far, mask, arrived.at[0]),
        pltpu.make_async_copy(table_far, table, arrived.at[1]),
    ]
    large = [
        [
            pltpu.make_async_copy(far.at[:, part], near.at[:, part], arrived.at[2 * n + which])
            for which, (far, near) in enumerate(((wave_far, wave), (speed_far, speed)))
        ]
        for n, part in enumerate(parts, 1)
    ]
    for copies in (small, *large):
        for copy in copies:
            copy.start()
    for copy in small:
        copy.wait()
    sea = mask[...].astype(jnp.float32)
    first_core = lax.axis_index("lon") % 2 == 0
    for part, copies in zip(parts, large):
        for copy in copies:
            copy.wait()
        cosine, east = table[0:1, part], table[2:3, part] > 0.5

        def row(i):
            water = sea[:, i : i + 1]
            flow = speed[i * lats : (i + 1) * lats, part] * cosine * water
            scale = 1.0 / (1.0 + flow)
            return flow * scale, wave[i * lats : (i + 1) * lats, part] * water * scale

        value = total = None
        for k in range(count):
            if k < count // 2:
                a_low, b_low = row(k)
                a_high, b_high = row(count - 1 - k)
                there = (count - 1 - k) * lats
                put(decay, rows, part, there, jnp.where(east, a_high, a_low))
                put(partial, rows, part, there, jnp.where(east, b_high, b_low))
                a, b = jnp.where(east, a_low, a_high), jnp.where(east, b_low, b_high)
            else:
                a = take(decay, rows, part, k * lats, lats)
                b = take(partial, rows, part, k * lats, lats)
            value = b if k == 0 else a * value + b
            total = a if k == 0 else a * total
            put(partial, rows, part, k * lats, value)
            put(decay, rows, part, k * lats, total)
        low, high = (
            jnp.concatenate([state[rows] for state in (total, value)], axis=0)
            for rows in (slice(0, lats // 2), slice(lats // 2, lats))
        )
        keep[:, part] = jnp.where(first_core, low, high)
        give[:, part] = jnp.where(first_core, high, low)


def lat_coefficients(speed, mask, edges, table, ratio, scaled, decay, whole, rate):
    count, lons = mask.shape
    rows = lons * count
    place, last = lax.axis_index("lat"), lax.axis_size("lat") - 1
    sea = mask[...].astype(jnp.float32).T
    opened = edges[...].astype(jnp.float32).T
    south = jnp.where(place == 0, opened[:, 0:1], 1.0)
    north = jnp.where(place == last, opened[:, 1:2], 1.0)
    for part in chunks(speed.shape[1]):
        put(rate, rows, part, 0, speed[:, part])
        sine, up = table[1:2, part], table[3:4, part] > 0.5
        flows = [
            take(rate, rows, part, j, lons, count) * sine * sea[:, j : j + 1] for j in range(count)
        ]
        total = None
        for k in range(count):
            flow = jnp.where(up, flows[k], flows[count - 1 - k])
            shown = flow * jnp.where(up, south, north) if k == 0 else flow
            scale = 1.0 / (1.0 + shown)
            a = flow * scale
            total = a if k == 0 else a * total
            put(ratio, rows, part, k * lons, a)
            put(scaled, rows, part, k * lons, scale)
            put(decay, rows, part, k * lons, total)
        whole[:, part] = total


def ordered_group(own, received, place, positive, wanted=()):
    members = [own, *received]
    in_place = []
    for slot in range(4):
        value = members[0]
        for d in range(1, 4):
            hit = place ^ slot == d
            value = [jnp.where(hit, new, old) for new, old in zip(members[d], value)]
        in_place.append(value)
    swept = [
        [jnp.where(positive, low, high) for low, high in zip(in_place[slot], in_place[3 - slot])]
        for slot in range(4)
    ]
    prefixes = [[jnp.ones_like(own[0]), jnp.zeros_like(own[1])], swept[0]]
    prefixes.append(compose(swept[0], swept[1]))
    prefixes.append(compose(prefixes[2], swept[2]))
    whole = compose(prefixes[3], swept[3])

    def chosen(index):
        value = prefixes[0]
        for slot in range(1, 4):
            value = [jnp.where(index == slot, new, old) for new, old in zip(prefixes[slot], value)]
        return value

    return whole, *(
        [jnp.where(positive, low, high) for low, high in zip(chosen(at), chosen(3 - at))]
        for at in wanted or (place,)
    )


def halves(ref, part):
    rows = ref.shape[0] // 2
    return [ref[0:rows, part], ref[rows : 2 * rows, part]]


def store(ref, part, state):
    rows = ref.shape[0] // 2
    ref[0:rows, part], ref[rows : 2 * rows, part] = state


def lon_group(own, first, second, third, table, whole, before, before_partner):
    place = lax.axis_index("lon") % 4
    for part in chunks(own.shape[1]):
        received = [halves(ref, part) for ref in (first, second, third)]
        states = ordered_group(
            halves(own, part), received, place, table[2:3, part] > 0.5, (place, place ^ 1)
        )
        for ref, state in zip((whole, before, before_partner), states):
            store(ref, part, state)


def lon_cycle(own, first, second, third, before, before_partner, table, keep, give):
    place = lax.axis_index("lon") // 4
    for part in chunks(own.shape[1]):
        received = [halves(ref, part) for ref in (first, second, third)]
        cycle, start = ordered_group(halves(own, part), received, place, table[2:3, part] > 0.5)
        entering = cycle[1] / (1.0 - cycle[0])
        entering = start[0] * entering + start[1]
        for ref, state in ((keep, before), (give, before_partner)):
            a, b = halves(state, part)
            ref[:, part] = a * entering + b


def lon_finish(partial, decay, kept, given, ratio, scaled, table, message, solved, half):
    lats, lons = 2 * kept.shape[0], message.shape[0]
    rows = lons * lats
    first_core = lax.axis_index("lon") % 2 == 0
    for part in chunks(kept.shape[1]):
        east, up = table[2:3, part] > 0.5, table[3:4, part] > 0.5
        mine, other = kept[:, part], given[:, part]
        entering = jnp.concatenate(
            [jnp.where(first_core, mine, other), jnp.where(first_core, other, mine)], axis=0
        )
        for k in range(lons // 2):
            low, high = k * lats, (lons - 1 - k) * lats
            a, b = (
                take(partial, rows, part, at, lats) + take(decay, rows, part, at, lats) * entering
                for at in (low, high)
            )
            put(half, rows, part, low, jnp.where(east, a, b))
            put(half, rows, part, high, jnp.where(east, b, a))
        lines = [take(half, rows, part, j, lons, lats) for j in range(lats)]
        value = None
        for k in range(lats):
            step = take(scaled, rows, part, k * lons, lons)
            step = step * jnp.where(up, lines[k], lines[lats - 1 - k])
            value = step if k == 0 else take(ratio, rows, part, k * lons, lons) * value + step
            put(solved, rows, part, k * lons, value)
        message[:, part] = value


def packed(value, positive):
    rows = value.shape[0] // 2
    low, high = value[0:rows], pltpu.roll(value[rows : 2 * rows], HALF, 1)
    return jnp.where(positive, low, high), jnp.where(positive, high, low)


def unpacked(message):
    bins = message.shape[1]
    return jnp.concatenate([message, pltpu.roll(message, bins - HALF, 1)], axis=0)


def lat_group_ahead(own, first, second, third, table, *messages):
    row = lax.axis_index("lat") // 4
    total = own[...] * first[...] * second[...] * third[...]
    north, south = packed(total, table[3:4, :] > 0.5)
    for d, message in enumerate(messages, 1):
        message[...] = jnp.where(row ^ d > row, north, south)


def lat_group(own, own_ahead, first, second, third, *rest):
    *ahead, table, before, message_1, message_2, message_3 = rest
    place = lax.axis_index("lat")
    row = place // 4
    rows = own.shape[0]
    received = [[a[...], b[...]] for a, b in zip(ahead, (first, second, third))]
    up = table[3:4, :] > 0.5
    total, prefix = ordered_group([own_ahead[...], own[...]], received, place % 4, up)
    before[0:rows], before[rows : 2 * rows] = prefix
    north, south = packed(total[1], up)
    for d, message in enumerate((message_1, message_2, message_3), 1):
        message[...] = jnp.where(row ^ d > row, north, south)


def lat_finish(
    solved, decay, before, first, second, third, ahead_1, ahead_2, ahead_3, table, out, result, sent
):
    lons, bins = before.shape[0] // 2, before.shape[1]
    rows = out.shape[0]
    count = rows // lons
    row = lax.axis_index("lat") // 4
    up = table[3:4, :] > 0.5
    received = [
        [unpacked(a[...]), unpacked(b[...])]
        for a, b in zip((ahead_1, ahead_2, ahead_3), (first, second, third))
    ]

    def from_row(source):
        value = received[0]
        for d in (2, 3):
            value = [jnp.where(row ^ source == d, new, old) for new, old in zip(received[d - 1], value)]
        return value

    entering = jnp.zeros_like(received[0][0])
    for n in range(3):
        a, b = (jnp.where(up, x, y) for x, y in zip(from_row(n), from_row(3 - n)))
        reached = jnp.where(up, (n < row).astype(jnp.float32), (3 - n > row).astype(jnp.float32))
        entering = jnp.where(reached > 0.5, a * entering + b, entering)
    entering = before[0:lons] * entering + before[lons : 2 * lons]
    copies = []
    for part in chunks(bins):
        goes_up, inflow = up[:, part], entering[:, part]
        for k in range(count // 2):
            low, high = k * lons, (count - 1 - k) * lons
            a, b = (
                take(solved, rows, part, at, lons) + take(decay, rows, part, at, lons) * inflow
                for at in (low, high)
            )
            put(result, rows, part, k, jnp.where(goes_up, a, b), count)
            put(result, rows, part, count - 1 - k, jnp.where(goes_up, b, a), count)
        for tile in tiles_of(part):
            copy = pltpu.make_async_copy(
                result.at[pl.ds(tile * rows, rows), :],
                out.at[:, pl.ds(tile * LANES, LANES)],
                sent.at[tile],
            )
            copy.start()
            copies.append(copy)
    for copy in copies:
        copy.wait()


def run(kernel, shapes, *operands, scratch=(), far_inputs=(), far_outputs=()):
    here, away = pl.BlockSpec(memory_space=pltpu.VMEM), pl.BlockSpec(memory_space=pltpu.HBM)
    operands = [
        pltpu.with_memory_space_constraint(x, pltpu.HBM) if n in far_inputs else x
        for n, x in enumerate(operands)
    ]
    return pl.pallas_call(
        kernel,
        out_shape=[jax.ShapeDtypeStruct(shape, jnp.float32) for shape in shapes],
        in_specs=[away if n in far_inputs else here for n in range(len(operands))],
        out_specs=[away if n in far_outputs else here for n in range(len(shapes))],
        scratch_shapes=scratch,
        compiler_params=pltpu.CompilerParams(vmem_limit_bytes=8 << 20),
        name=kernel.__name__,
    )(*operands)


NEAR = [[i ^ d for i in range(16)] for d in (1, 2, 3)]
FAR = [[i ^ d for i in range(16)] for d in (4, 8, 12)]
FAR_LON = [[i ^ d for i in range(16)] for d in (4, 10, 12)]


def exchange(values, axis, sources):
    return [
        lax.ppermute(value, axis, [(source, i) for i, source in enumerate(places)])
        for value, places in zip(values, sources)
    ]


def body(wave_action, lon_speed, lat_speed, land_mask, open_edges):
    lons, lats, bins = wave_action.shape
    table = jnp.asarray(bin_tables(bins))
    flat = (lons * lats, bins)
    wave, speed, lat_rate = (x.reshape(flat) for x in (wave_action, lon_speed, lat_speed))
    small, large = (lats, bins), (2 * lons, bins)

    tiled = (bins // LANES * lons * lats, LANES)
    buffer = pltpu.VMEM(tiled, jnp.float32)
    signals = pltpu.SemaphoreType.DMA((bins // LANES,))

    sea = land_mask.T
    keep, give, partial, decay = run(
        lon_local, [small, small, tiled, tiled], wave, speed, sea, table,
        scratch=[
            pltpu.VMEM(flat, jnp.float32), pltpu.VMEM(flat, jnp.float32),
            pltpu.VMEM(sea.shape, sea.dtype), pltpu.VMEM(table.shape, table.dtype),
            pltpu.SemaphoreType.DMA((2 + 2 * len(chunks(bins)),)),
        ],
        far_inputs=range(4),
    )
    near = exchange([give, keep, give], "lon", NEAR)
    ratio, scaled, lat_decay, lat_ahead = run(
        lat_coefficients, [tiled] * 3 + [(lons, bins)], lat_rate, sea, open_edges, table,
        scratch=[buffer],
    )
    near_ahead = exchange([lat_ahead] * 3, "lat", NEAR)
    whole, before, before_partner = run(lon_group, [small] * 3, keep, *near, table)
    far = exchange([whole] * 3, "lon", FAR_LON)
    half = (lons // 2, bins)
    far_ahead = exchange(
        run(lat_group_ahead, [half] * 3, lat_ahead, *near_ahead, table), "lat", FAR
    )
    inflow = (lats // 2, bins)
    kept, give = run(
        lon_cycle, [inflow, inflow], whole, *far, before, before_partner, table
    )
    given = lax.ppermute(give, "lon", [(i ^ 1, i) for i in range(16)])
    lat_own, solved = run(
        lon_finish, [(lons, bins), tiled], partial, decay, kept, given, ratio, scaled, table,
        scratch=[buffer],
    )
    near = exchange([lat_own] * 3, "lat", NEAR)
    lat_before, *sends = run(
        lat_group, [large, *[half] * 3], lat_own, lat_ahead, *near, *near_ahead, table
    )
    far = exchange(sends, "lat", FAR)
    (out,) = run(
        lat_finish, [flat], solved, lat_decay, lat_before, *far, *far_ahead, table,
        scratch=[buffer, signals], far_outputs=(0,),
    )
    return out.reshape(wave_action.shape)


def solution(mesh):
    return jax.shard_map(
        body,
        mesh=mesh,
        in_specs=(
            P("lon", "lat", None),
            P("lon", "lat", None),
            P("lon", "lat", None),
            P("lon", "lat"),
            P(None, "lon"),
        ),
        out_specs=P("lon", "lat", None),
        check_vma=False,
    )
```
